8 devices in a mesh: rep: 1 (over z), r: 2 (over y), s: 4 (over x, core).
Axes of the slice: x: 2, y: 2, z: 1, core: 2. Of those that a mesh axis runs over, the one named last changes fastest.
Arguments:
- x: bfloat16 [8, 4096, 896], P(('rep', 'r', 's'))
- dy: bfloat16 [8, 4096, 896], P(('rep', 'r', 's'))
- w_gate: bfloat16 [2, 896, 2560], P(None, 's')
- w_up: bfloat16 [2, 896, 2560], P(None, 's')
- w_down: bfloat16 [2, 2560, 896], P(None, 's')
Outputs:
- output 1: bfloat16 [8, 4096, 896], P(('rep', 'r', 's'))
- output 2: bfloat16 [2, 896, 2560], P('rep', 's')
- output 3: bfloat16 [2, 896, 2560], P('rep', 's')
- output 4: bfloat16 [2, 2560, 896], P('rep', 's')
All inputs are finite; a program needn't handle non-finite values.
Results may differ from the reference program's by a relative error of at most 0.018.
Values are sent between devices in bfloat16 or wider.
A program may use at most 2 GiB of HBM per device.

```python
import jax
import jax.numpy as jnp
from jax import lax

SEQUENCES = 8
TOKENS = 4096
D = 896
FF = 2560
LAYERS = 2
NAMES = ("w_gate", "w_up", "w_down")
SHAPES = {"w_gate": (LAYERS, D, FF), "w_up": (LAYERS, D, FF), "w_down": (LAYERS, FF, D)}


def bump(key, n, height):
    away = (jnp.arange(n, dtype=jnp.int32) - jax.random.randint(key, (), 0, n, jnp.int32)) % n
    return jnp.where(away < n // 8, height, 1.0)


def together(key, own, strength):
    shared = jax.random.normal(key, own.shape[1:], jnp.float32)
    return (own + strength * shared) * lax.rsqrt(1 + strength * strength)


def setup_inputs(seed: int = 0, part: int = 0) -> dict:
    kx, kdy, ka, kb, kz, kf, kh, kl, *kw = jax.random.split(jax.random.key(seed), 8 + len(NAMES))
    kx, kdy, ka, kb = (jax.random.fold_in(k, part) for k in (kx, kdy, ka, kb))
    shape = (SEQUENCES, TOKENS, D)
    much_x, much_dy = jax.random.uniform(kz, (2,), jnp.float32, 0.0, 1.0)
    layers = 2.0 ** jax.random.uniform(kl, (LAYERS, 1, 1), jnp.float32, -1.0, 1.0)
    x = together(ka, jax.random.normal(kx, shape, jnp.float32), much_x) * bump(kf, D, 4.0)
    dy = together(kb, jax.random.normal(kdy, shape, jnp.float32), much_dy)
    drawn = {"x": x.astype(jnp.bfloat16), "dy": (dy * (SEQUENCES * TOKENS) ** -0.5).astype(jnp.bfloat16)}
    for key, name in zip(kw, NAMES, strict=True):
        w = jax.random.normal(key, SHAPES[name], jnp.float32) * SHAPES[name][1] ** -0.5
        drawn[name] = (w * {"w_gate": 1.0, "w_up": bump(kh, FF, 4.0), "w_down": layers}[name]).astype(jnp.bfloat16)
    return drawn


def matmul(a, w):
    return jnp.dot(a, w, preferred_element_type=jnp.float32).astype(jnp.bfloat16)


def normed(h):
    wide = h.astype(jnp.float32)
    scale = lax.rsqrt(jnp.mean(wide**2, -1, keepdims=True) + 1e-6)
    return (wide * scale).astype(jnp.bfloat16)


def layer(h, w):
    a = normed(h)
    gate = jnp.dot(a, w["w_gate"], preferred_element_type=jnp.float32)
    up = jnp.dot(a, w["w_up"], preferred_element_type=jnp.float32)
    return h + matmul((jax.nn.silu(gate) * up).astype(jnp.bfloat16), w["w_down"])


def stack(weights, h):
    return lax.scan(lambda h, w: (layer(h, w), None), h, weights)[0]


def reference(x, dy, w_gate, w_up, w_down):
    weights = dict(zip(NAMES, (w_gate, w_up, w_down), strict=True))

    def take(so_far, sequence):
        h, by_y = sequence
        _, back = jax.vjp(stack, weights, h)
        by_weights, by_h = back(by_y)
        return jax.tree.map(lambda total, term: total + term.astype(jnp.float32), so_far, by_weights), by_h

    none_yet = {name: jnp.zeros(w.shape, jnp.float32) for name, w in weights.items()}
    by_weights, by_x = lax.scan(take, none_yet, (x, dy))
    return (by_x, *(by_weights[name].astype(jnp.bfloat16) for name in NAMES))
```

```python
import functools

import jax
import jax.numpy as jnp
from jax import lax
from jax.experimental import pallas as pl
from jax.experimental.pallas import tpu as pltpu
from jax.sharding import PartitionSpec as P

F32, BF16 = jnp.float32, jnp.bfloat16
ANY = pl.BlockSpec(memory_space=pl.ANY)
TILE = 512
CHUNK = 1024
SUB = 512
EDGE = 256
EPS = 1e-6


def dot(a, b, over=(1, 0)):
    return lax.dot_general(a, b, (((over[0],), (over[1],)), ((), ())), preferred_element_type=F32)


def at(step, size):
    return pl.ds(pl.multiple_of(step * size, size), size)


def scale_of(h):
    return lax.rsqrt(jnp.mean(h * h, 0, keepdims=True) + EPS)


def turned(source, stage, sems, write):
    chunks = source.shape[0] // EDGE

    def copy(c, slot):
        return pltpu.make_async_copy(source.at[at(c, EDGE), :], stage.at[slot], sems.at[slot])

    copy(0, 0).start()
    copy(1, 1).start()

    def step(c, _):
        for slot in range(2):
            copy(2 * c + slot, slot).wait()
            write(2 * c + slot, stage[slot].T)

            @pl.when(2 * c + slot + 2 < chunks)
            def _():
                copy(2 * c + slot + 2, slot).start()
        return 0

    lax.fori_loop(0, chunks // 2, step, 0)


def forward_kernel(x, wg, wu, wd, xt_out, at_out, ht_out, at1_out, xt, a, total, p, stage, sems, osems):
    n, passes = pl.program_id(0), pl.num_programs(0)
    chunks = a.shape[1] // CHUNK

    @pl.when(n == 0)
    def _():
        def write(c, ht):
            h = ht.astype(F32)
            xt[:, at(c, EDGE)] = ht
            a[:, at(c, EDGE)] = (h * scale_of(h)).astype(BF16)

        turned(x, stage, sems, write)
        pltpu.make_async_copy(xt, xt_out, osems.at[0]).start()
        pltpu.make_async_copy(a, at_out, osems.at[1]).start()
        total[...] = jnp.zeros_like(total)

    def step(c, _):
        for i in range(CHUNK // SUB):
            tokens = pl.ds(pl.multiple_of(c * CHUNK + i * SUB, SUB), SUB)
            g, u = dot(wg[...], a[:, tokens], (0, 0)), dot(wu[...], a[:, tokens], (0, 0))
            p[:, pl.ds(i * SUB, SUB)] = (g * jax.nn.sigmoid(g) * u).astype(BF16)
        total[:, at(c, CHUNK)] += dot(wd[...], p[...], (0, 0))
        return 0

    lax.fori_loop(0, chunks, step, 0)

    @pl.when(n == passes - 1)
    def _():
        pltpu.make_async_copy(xt, xt_out, osems.at[0]).wait()
        pltpu.make_async_copy(a, at_out, osems.at[1]).wait()

        def last(c, _):
            cols = at(c, EDGE)
            h = (xt[:, cols].astype(F32) + total[:, cols].astype(BF16).astype(F32)).astype(BF16)
            xt[:, cols] = h
            h = h.astype(F32)
            a[:, cols] = (h * scale_of(h)).astype(BF16)
            return 0

        lax.fori_loop(0, a.shape[1] // EDGE, last, 0)
        one = pltpu.make_async_copy(xt, ht_out, osems.at[0])
        two = pltpu.make_async_copy(a, at1_out, osems.at[1])
        one.start(), two.start(), one.wait(), two.wait()


def forward(x, wg, wu, wd):
    tokens, d = x.shape
    state = jax.ShapeDtypeStruct((d, tokens), BF16)
    return pl.pallas_call(
        forward_kernel,
        grid=(wg.shape[1] // TILE,),
        in_specs=[ANY, pl.BlockSpec((d, TILE), lambda n: (0, n)), pl.BlockSpec((d, TILE), lambda n: (0, n)), pl.BlockSpec((TILE, d), lambda n: (n, 0))],
        out_specs=[ANY] * 4,
        out_shape=[state] * 4,
        scratch_shapes=[
            pltpu.VMEM((d, tokens), BF16),
            pltpu.VMEM((d, tokens), BF16),
            pltpu.VMEM((d, tokens), F32),
            pltpu.VMEM((TILE, CHUNK), BF16),
            pltpu.VMEM((2, EDGE, d), BF16),
            pltpu.SemaphoreType.DMA((2,)),
            pltpu.SemaphoreType.DMA((2,)),
        ],
        compiler_params=pltpu.CompilerParams(vmem_limit_bytes=63 * 2**20, dimension_semantics=("arbitrary",)),
        cost_estimate=pl.CostEstimate(flops=6 * tokens * d * wg.shape[1], bytes_accessed=60 * 2**20, transcendentals=0),
        name="forward_layer",
    )(x, wg, wu, wd)


def backward_kernel(turn_in, turn_out, at_in, ht_in, by_in, wg, wu, wd, og, ou, od, by_out, a, by, total, accg, accu, accd, p, dg, du, stage, sems, osems):
    n, passes = pl.program_id(0), pl.num_programs(0)
    chunks = a.shape[1] // CHUNK

    @pl.when(n == 0)
    def _():
        one = pltpu.make_async_copy(at_in, a, osems.at[0])
        one.start()
        if turn_in:
            def write(c, t):
                by[:, at(c, EDGE)] = t

            turned(by_in, stage, sems, write)
        else:
            two = pltpu.make_async_copy(by_in, by, osems.at[1])
            two.start()
            two.wait()
        total[...] = jnp.zeros_like(total)
        one.wait()

    accg[...] = jnp.zeros_like(accg)
    accu[...] = jnp.zeros_like(accu)
    accd[...] = jnp.zeros_like(accd)

    def step(c, _):
        cols = at(c, CHUNK)
        for i in range(CHUNK // SUB):
            tokens, q = pl.ds(pl.multiple_of(c * CHUNK + i * SUB, SUB), SUB), pl.ds(i * SUB, SUB)
            g, u = dot(wg[...], a[:, tokens], (0, 0)), dot(wu[...], a[:, tokens], (0, 0))
            dp = dot(wd[...], by[:, tokens]).astype(BF16).astype(F32)
            sg = jax.nn.sigmoid(g)
            s = g * sg
            p[:, q] = (s * u).astype(BF16)
            du[:, q] = (dp * s).astype(BF16)
            dg[:, q] = (dp * u * (sg + s * (1 - sg))).astype(BF16)
        total[:, cols] += dot(wg[...], dg[...]) + dot(wu[...], du[...])
        accg[...] += dot(a[:, cols], dg[...], (1, 1))
        accu[...] += dot(a[:, cols], du[...], (1, 1))
        accd[...] += dot(by[:, cols], p[...], (1, 1))
        return 0

    lax.fori_loop(0, chunks, step, 0)
    og[...] = accg[...].astype(BF16)
    ou[...] = accu[...].astype(BF16)
    od[...] = accd[...].T.astype(BF16)

    @pl.when(n == passes - 1)
    def _():
        one = pltpu.make_async_copy(ht_in, a, osems.at[0])
        one.start()
        one.wait()

        def changed(cols):
            da, h = total[:, cols].astype(BF16).astype(F32), a[:, cols].astype(F32)
            f = scale_of(h)
            dh = (f * da - h * (f * f * f * jnp.mean(da * h, 0, keepdims=True))).astype(BF16)
            return (by[:, cols].astype(F32) + dh.astype(F32)).astype(BF16)

        if turn_out:
            def copy(c, slot):
                return pltpu.make_async_copy(stage.at[slot], by_out.at[at(c, EDGE), :], sems.at[slot])

            def last(c, _):
                for slot in range(2):
                    @pl.when(c > 0)
                    def _():
                        copy(2 * c + slot - 2, slot).wait()

                    stage[slot] = changed(at(2 * c + slot, EDGE)).T
                    copy(2 * c + slot, slot).start()
                return 0

            steps = a.shape[1] // EDGE
            lax.fori_loop(0, steps // 2, last, 0)
            copy(steps - 2, 0).wait()
            copy(steps - 1, 1).wait()
        else:
            def last(c, _):
                by[:, at(c, EDGE)] = changed(at(c, EDGE))
                return 0

            lax.fori_loop(0, a.shape[1] // EDGE, last, 0)
            two = pltpu.make_async_copy(by, by_out, osems.at[1])
            two.start()
            two.wait()


def backward(a, h, by, wg, wu, wd, turn_in, turn_out):
    d, tokens = a.shape
    wide, tall = pl.BlockSpec((d, TILE), lambda n: (0, n)), pl.BlockSpec((TILE, d), lambda n: (n, 0))
    return pl.pallas_call(
        functools.partial(backward_kernel, turn_in, turn_out),
        grid=(wg.shape[1] // TILE,),
        in_specs=[ANY, ANY, ANY, wide, wide, tall],
        out_specs=[wide, wide, tall, ANY],
        out_shape=[jax.ShapeDtypeStruct(w.shape, BF16) for w in (wg, wu, wd)] + [jax.ShapeDtypeStruct((tokens, d) if turn_out else (d, tokens), BF16)],
        scratch_shapes=[
            pltpu.VMEM((d, tokens), BF16),
            pltpu.VMEM((d, tokens), BF16),
            pltpu.VMEM((d, tokens), F32),
            pltpu.VMEM((d, TILE), F32),
            pltpu.VMEM((d, TILE), F32),
            pltpu.VMEM((d, TILE), F32),
            pltpu.VMEM((TILE, CHUNK), BF16),
            pltpu.VMEM((TILE, CHUNK), BF16),
            pltpu.VMEM((TILE, CHUNK), BF16),
            pltpu.VMEM((2, EDGE, d), BF16),
            pltpu.SemaphoreType.DMA((2,)),
            pltpu.SemaphoreType.DMA((2,)),
        ],
        compiler_params=pltpu.CompilerParams(vmem_limit_bytes=63 * 2**20, dimension_semantics=("arbitrary",)),
        cost_estimate=pl.CostEstimate(flops=16 * tokens * d * wg.shape[1], bytes_accessed=60 * 2**20, transcendentals=0),
        name="backward_layer",
    )(a, h, by, wg, wu, wd)


def solution(mesh):
    def step(x, dy, *weights):
        def fetched(number):
            return [lax.all_gather(w[number], "s", axis=0, tiled=True) for w in weights]

        def summed(term):
            return lax.psum(lax.psum_scatter(term, "s", scatter_dimension=0, tiled=True), "r")

        first, last = fetched(0), fetched(1)
        xt, a0, h1, a1 = forward(x[0], *first)
        *by_w1, by_h1 = backward(a1, h1, dy[0], *last, turn_in=True, turn_out=False)
        *by_w0, by_x = backward(a0, xt, by_h1, *first, turn_in=False, turn_out=True)
        mine = [[summed(t) for t in by_w0], [summed(t) for t in by_w1]]
        return (by_x[None], *(jnp.stack([mine[0][i], mine[1][i]]) for i in range(3)))

    states, cut = P(("rep", "r", "s"), None, None), P(None, "s", None)
    return jax.shard_map(
        step,
        mesh=mesh,
        in_specs=(states, states) + (cut,) * 3,
        out_specs=(states,) + (P("rep", "s", None),) * 3,
        check_vma=False,
    )
```

```python
import functools

import jax
import jax.numpy as jnp
from jax import lax
from jax.experimental import pallas as pl
from jax.experimental.pallas import tpu as pltpu
from jax.sharding import PartitionSpec as P

F32, BF16 = jnp.float32, jnp.bfloat16
ANY = pl.BlockSpec(memory_space=pl.ANY)
TILE = 512
CHUNK = 1024
SUB = 512
EDGE = 256
EPS = 1e-6
BLOCK = 2688
HALF = BLOCK // 2
MESH = pl.DeviceIdType.MESH


def dot(a, b, over=(1, 0)):
    return lax.dot_general(a, b, (((over[0],), (over[1],)), ((), ())), preferred_element_type=F32)


def flat(w):
    return w[...].reshape(-1, w.shape[-1])


def tiles_of(w):
    return pl.BlockSpec((w.shape[0], None, *w.shape[2:]), lambda n: (0, n, 0, 0))


def at(step, size):
    return pl.ds(pl.multiple_of(step * size, size), size)


def scale_of(h):
    return lax.rsqrt(jnp.mean(h * h, 0, keepdims=True) + EPS)


def turned(source, stage, sems, write):
    chunks = source.shape[0] // EDGE

    def copy(c, slot):
        return pltpu.make_async_copy(source.at[at(c, EDGE), :], stage.at[slot], sems.at[slot])

    copy(0, 0).start()
    copy(1, 1).start()

    def step(c, _):
        for slot in range(2):
            copy(2 * c + slot, slot).wait()
            write(2 * c + slot, stage[slot].T)

            @pl.when(2 * c + slot + 2 < chunks)
            def _():
                copy(2 * c + slot + 2, slot).start()
        return 0

    lax.fori_loop(0, chunks // 2, step, 0)


def forward_kernel(x, wg, wu, wd, xt_out, at_out, ht_out, at1_out, xt, a, total, p, stage, sems, osems):
    n, passes = pl.program_id(0), pl.num_programs(0)
    chunks = a.shape[1] // CHUNK

    @pl.when(n == 0)
    def _():
        def write(c, ht):
            h = ht.astype(F32)
            xt[:, at(c, EDGE)] = ht
            a[:, at(c, EDGE)] = (h * scale_of(h)).astype(BF16)

        turned(x, stage, sems, write)
        pltpu.make_async_copy(xt, xt_out, osems.at[0]).start()
        pltpu.make_async_copy(a, at_out, osems.at[1]).start()
        total[...] = jnp.zeros_like(total)

    def step(c, _):
        for i in range(CHUNK // SUB):
            tokens = pl.ds(pl.multiple_of(c * CHUNK + i * SUB, SUB), SUB)
            g, u = dot(flat(wg), a[:, tokens], (0, 0)), dot(flat(wu), a[:, tokens], (0, 0))
            p[:, pl.ds(i * SUB, SUB)] = (g * jax.nn.sigmoid(g) * u).astype(BF16)
        total[:, at(c, CHUNK)] += dot(flat(wd), p[...], (0, 0))
        return 0

    lax.fori_loop(0, chunks, step, 0)

    @pl.when(n == passes - 1)
    def _():
        pltpu.make_async_copy(xt, xt_out, osems.at[0]).wait()
        pltpu.make_async_copy(a, at_out, osems.at[1]).wait()

        def last(c, _):
            cols = at(c, EDGE)
            h = (xt[:, cols].astype(F32) + total[:, cols].astype(BF16).astype(F32)).astype(BF16)
            xt[:, cols] = h
            h = h.astype(F32)
            a[:, cols] = (h * scale_of(h)).astype(BF16)
            return 0

        lax.fori_loop(0, a.shape[1] // EDGE, last, 0)
        one = pltpu.make_async_copy(xt, ht_out, osems.at[0])
        two = pltpu.make_async_copy(a, at1_out, osems.at[1])
        one.start(), two.start(), one.wait(), two.wait()


def forward(x, wg, wu, wd):
    tokens, d = x.shape
    state = jax.ShapeDtypeStruct((d, tokens), BF16)
    return pl.pallas_call(
        forward_kernel,
        grid=(wg.shape[1],),
        in_specs=[ANY, *map(tiles_of, (wg, wu, wd))],
        out_specs=[ANY] * 4,
        out_shape=[state] * 4,
        scratch_shapes=[
            pltpu.VMEM((d, tokens), BF16),
            pltpu.VMEM((d, tokens), BF16),
            pltpu.VMEM((d, tokens), F32),
            pltpu.VMEM((TILE, CHUNK), BF16),
            pltpu.VMEM((2, EDGE, d), BF16),
            pltpu.SemaphoreType.DMA((2,)),
            pltpu.SemaphoreType.DMA((2,)),
        ],
        compiler_params=pltpu.CompilerParams(vmem_limit_bytes=63 * 2**20, dimension_semantics=("arbitrary",)),
        cost_estimate=pl.CostEstimate(flops=6 * tokens * d * TILE * wg.shape[1], bytes_accessed=60 * 2**20, transcendentals=0),
        name="forward_layer",
    )(x, wg, wu, wd)


def backward_kernel(final, *refs):
    refs = iter(refs)
    take = lambda count: [next(refs) for _ in range(count)]
    at_in, ht_in, by_in, wg, wu, wd = take(6)
    if final:
        kept_in, sent_in = take(2)
        by_out, sums_out = take(2)
    else:
        by_out, sums_out, kept_out, sent_out = take(4)
    a, by, total, accg, accu, accd, p, dg, du, stage = take(10)
    kept, send_d, recv_d, send_x, recv_x, send_y, recv_y, done = take(8)
    sems, osems, ssem, rsem, free = take(5)

    n, passes = pl.program_id(0), pl.num_programs(0)
    chunks, steps = a.shape[1] // CHUNK, a.shape[1] // EDGE
    s, r = lax.axis_index("s"), lax.axis_index("r")
    x, core = s // 2, s % 2
    partner, across, beside = {"s": s + 1 - 2 * core}, {"s": (s + 2) % 4}, {"r": 1 - r}
    jobs = 6 if final else 4
    mine, other = pl.ds(pl.multiple_of(r * HALF, HALF), HALF), pl.ds(pl.multiple_of((1 - r) * HALF, HALF), HALF)

    def remote(number, source, target, device):
        return pltpu.make_async_remote_copy(source, target, ssem.at[number], rsem.at[number], device_id=device, device_id_type=MESH)

    to_partner = remote(0, send_d, recv_d, partner)
    to_across = remote(1, send_x, recv_x, across)
    to_beside = remote(2, send_y, recv_y, beside)
    back_beside = remote(3, done.at[mine, :], done.at[mine, :], beside)
    devices = (partner, across, beside, beside)

    def send(number, copy, job):
        @pl.when(job > 0)
        def _():
            pl.semaphore_wait(free.at[number], 1)

        copy.start()

    def freed(number, job):
        @pl.when(job < jobs - 1)
        def _():
            pl.semaphore_signal(free.at[number], 1, device_id=devices[number], device_id_type=MESH)

    def cut(owner, write):
        rows = pl.ds(pl.multiple_of(owner * 224, 32), 224)
        for k in range(4):
            write(k * 224, 224, accg[rows, k * 128 : k * 128 + 128])
            write(896 + k * 224, 224, accu[rows, k * 128 : k * 128 + 128])
        write(1792, 896, accd[:, pl.ds(pl.multiple_of(owner * 128, 128), 128)])

    def pack():
        for slot, place in ((0, x), (1, 1 - x)):
            def keep(first, size, value, slot=slot):
                kept[slot, first : first + size, :] = value

            def leave(first, size, value, slot=slot):
                send_d[slot, first : first + size, :] = value.astype(BF16)

            cut(2 * place + core, keep)
            cut(2 * place + 1 - core, leave)

    def after_partner(job):
        to_partner.wait_recv()
        to_partner.wait_send()
        send_x[...] = (kept[1] + recv_d[1].astype(F32)).astype(BF16)
        kept[0] = kept[0] + recv_d[0].astype(F32)
        freed(0, job)
        send(1, to_across, job)

    def after_across(job):
        to_across.wait_recv()
        to_across.wait_send()
        kept[0] = kept[0] + recv_x[...].astype(F32)
        send_y[...] = kept[0, other, :].astype(BF16)
        freed(1, job)
        send(2, to_beside, job)

    def after_beside(job):
        to_beside.wait_recv()
        to_beside.wait_send()
        done[mine, :] = (kept[0, mine, :] + recv_y[...].astype(F32)).astype(BF16)
        freed(2, job)
        send(3, back_beside, job)

    def written(job):
        return pltpu.make_async_copy(done, sums_out.at[job], osems.at[2])

    def whole(job):
        back_beside.wait_recv()
        back_beside.wait_send()
        written(job).start()

    def written_out(job):
        written(job).wait()
        freed(3, job)

    job = n if final else n - 1

    @pl.when(n == 0)
    def _():
        barrier = pltpu.get_barrier_semaphore()
        for device in (partner, across, beside):
            pl.semaphore_signal(barrier, 1, device_id=device, device_id_type=MESH)
        one = pltpu.make_async_copy(at_in, a, osems.at[0])
        one.start()
        if final:
            two = pltpu.make_async_copy(by_in, by, osems.at[1])
            two.start()
            three, four = pltpu.make_async_copy(kept_in, kept, sems.at[0]), pltpu.make_async_copy(sent_in, send_d, sems.at[1])
            three.start(), four.start()
            three.wait(), four.wait()
        pl.semaphore_wait(barrier, 3)
        if final:
            send(0, to_partner, job)
            two.wait()
        else:
            def write(c, t):
                by[:, at(c, EDGE)] = t

            turned(by_in, stage, sems, write)
        total[...] = jnp.zeros_like(total)
        one.wait()

    accg[...] = jnp.zeros_like(accg)
    accu[...] = jnp.zeros_like(accu)
    accd[...] = jnp.zeros_like(accd)

    def step(c, _):
        cols = at(c, CHUNK)
        gate, up, down = flat(wg), flat(wu), flat(wd)
        for i in range(CHUNK // SUB):
            tokens, q = pl.ds(pl.multiple_of(c * CHUNK + i * SUB, SUB), SUB), pl.ds(i * SUB, SUB)
            g, u = dot(gate, a[:, tokens], (0, 0)), dot(up, a[:, tokens], (0, 0))
            dp = dot(down, by[:, tokens]).astype(BF16).astype(F32)
            sg = jax.nn.sigmoid(g)
            t = g * sg
            p[:, q] = (t * u).astype(BF16)
            du[:, q] = (dp * t).astype(BF16)
            dg[:, q] = (dp * u * (sg + t * (1 - sg))).astype(BF16)
        total[:, cols] += dot(gate, dg[...]) + dot(up, du[...])
        accg[...] += dot(a[:, cols], dg[...], (1, 1))
        accu[...] += dot(a[:, cols], du[...], (1, 1))
        accd[...] += dot(by[:, cols], p[...], (1, 1))

        @pl.when((c == 0) & (job >= 0))
        def _():
            after_partner(job)

        @pl.when((c == 0) & (job >= 1))
        def _():
            whole(job - 1)

        @pl.when((c == 1) & (job >= 1))
        def _():
            written_out(job - 1)

        @pl.when((c == 2) & (job >= 0))
        def _():
            after_across(job)

        return 0

    lax.fori_loop(0, chunks, step, 0)

    @pl.when(job >= 0)
    def _():
        after_beside(job)

    pack()

    if final:
        send(0, to_partner, job + 1)
    else:
        @pl.when(n < passes - 1)
        def _():
            send(0, to_partner, job + 1)

    @pl.when(n == passes - 1)
    def _():
        one = pltpu.make_async_copy(ht_in, a, osems.at[0])
        one.start()
        if final:
            whole(4)
            after_partner(5)
        else:
            three, four = pltpu.make_async_copy(kept, kept_out, sems.at[0]), pltpu.make_async_copy(send_d, sent_out, sems.at[1])
            three.start(), four.start()
        one.wait()

        def changed(cols):
            da, h = total[:, cols].astype(BF16).astype(F32), a[:, cols].astype(F32)
            f = scale_of(h)
            dh = (f * da - h * (f * f * f * jnp.mean(da * h, 0, keepdims=True))).astype(BF16)
            return (by[:, cols].astype(F32) + dh.astype(F32)).astype(BF16)

        if final:
            def copy(c, slot):
                return pltpu.make_async_copy(stage.at[slot], by_out.at[at(c, EDGE), :], sems.at[slot])

            def last(c, _):
                for slot in range(2):
                    @pl.when(c > 0)
                    def _():
                        copy(2 * c + slot - 2, slot).wait()

                    stage[slot] = changed(at(2 * c + slot, EDGE)).T
                    copy(2 * c + slot, slot).start()
                return 0

            lax.fori_loop(0, steps // 2, last, 0)
            copy(steps - 2, 0).wait()
            copy(steps - 1, 1).wait()
            written_out(4)
            after_across(5)
            after_beside(5)
            whole(5)
            written_out(5)
        else:
            def last(c, _):
                by[:, at(c, EDGE)] = changed(at(c, EDGE))
                return 0

            lax.fori_loop(0, steps, last, 0)
            two = pltpu.make_async_copy(by, by_out, osems.at[1])
            two.start()
            whole(3)
            written_out(3)
            three.wait(), four.wait()
            two.wait()


def backward(a, h, by, wg, wu, wd, waiting=None):
    d, tokens = a.shape
    final = waiting is not None
    sums = lambda count: jax.ShapeDtypeStruct((count, BLOCK, 128), BF16)
    state = jax.ShapeDtypeStruct((tokens, d) if final else (d, tokens), BF16)
    handed = [] if final else [jax.ShapeDtypeStruct((2, BLOCK, 128), F32), sums(2)]
    return pl.pallas_call(
        functools.partial(backward_kernel, final),
        grid=(wg.shape[1],),
        in_specs=[ANY, ANY, ANY, *map(tiles_of, (wg, wu, wd))] + [ANY, ANY] * final,
        out_specs=[ANY] * (2 + len(handed)),
        out_shape=[state, sums(6 if final else 4), *handed],
        scratch_shapes=[
            pltpu.VMEM((d, tokens), BF16),
            pltpu.VMEM((d, tokens), BF16),
            pltpu.VMEM((d, tokens), F32),
            pltpu.VMEM((d, TILE), F32),
            pltpu.VMEM((d, TILE), F32),
            pltpu.VMEM((d, TILE), F32),
            pltpu.VMEM((TILE, CHUNK), BF16),
            pltpu.VMEM((TILE, CHUNK), BF16),
            pltpu.VMEM((TILE, CHUNK), BF16),
            pltpu.VMEM((2, EDGE, d), BF16),
            pltpu.VMEM((2, BLOCK, 128), F32),
            pltpu.VMEM((2, BLOCK, 128), BF16),
            pltpu.VMEM((2, BLOCK, 128), BF16),
            pltpu.VMEM((BLOCK, 128), BF16),
            pltpu.VMEM((BLOCK, 128), BF16),
            pltpu.VMEM((HALF, 128), BF16),
            pltpu.VMEM((HALF, 128), BF16),
            pltpu.VMEM((BLOCK, 128), BF16),
            pltpu.SemaphoreType.DMA((2,)),
            pltpu.SemaphoreType.DMA((3,)),
            pltpu.SemaphoreType.DMA((4,)),
            pltpu.SemaphoreType.DMA((4,)),
            pltpu.SemaphoreType.REGULAR((4,)),
        ],
        compiler_params=pltpu.CompilerParams(
            vmem_limit_bytes=63 * 2**20, dimension_semantics=("arbitrary",), collective_id=1 + final, has_side_effects=True
        ),
        cost_estimate=pl.CostEstimate(flops=16 * tokens * d * TILE * wg.shape[1], bytes_accessed=60 * 2**20, transcendentals=0),
        name="backward_final" if final else "backward_layer",
    )(a, h, by, wg, wu, wd, *(waiting or ()))


def solution(mesh):
    def step(x, dy, *weights):
        def cut(w):
            return w.reshape(w.shape[0], 4, 5, 128).transpose(2, 0, 1, 3).reshape(5, w.shape[0], 512)

        def fetched(number):
            gate, up, down = (w[number] for w in weights)
            return [lax.all_gather(w, "s") for w in (cut(gate), cut(up), down.reshape(5, 128, down.shape[1]))]

        def joined(tiles):
            wide = lambda t: t.reshape(5, 4, 224, 128).transpose(2, 1, 0, 3).reshape(224, 2560)
            return wide(tiles[:, :896]), wide(tiles[:, 896:1792]), tiles[:, 1792:].transpose(0, 2, 1).reshape(640, 896)

        first, last = fetched(0), fetched(1)
        xt, a0, h1, a1 = forward(x[0], *first)
        by_h1, early, *waiting = backward(a1, h1, dy[0], *last)
        by_x, late = backward(a0, xt, by_h1, *first, waiting)
        layers = joined(late[1:]), joined(jnp.concatenate([early, late[:1]]))
        return (by_x[None], *(jnp.stack([layer[i] for layer in layers]) for i in range(3)))

    states, cut = P(("rep", "r", "s"), None, None), P(None, "s", None)
    return jax.shard_map(
        step,
        mesh=mesh,
        in_specs=(states, states) + (cut,) * 3,
        out_specs=(states,) + (P("rep", "s", None),) * 3,
        check_vma=False,
    )
```

```python
import functools

import jax
import jax.numpy as jnp
from jax import lax
from jax.experimental import pallas as pl
from jax.experimental.pallas import tpu as pltpu
from jax.sharding import PartitionSpec as P

F32, BF16 = jnp.float32, jnp.bfloat16
ANY = pl.BlockSpec(memory_space=pl.ANY)
TILE = 512
CHUNK = 1024
SUB = 512
EDGE = 256
EPS = 1e-6
TN, NT = (0, 0), (1, 1)
PAIR = pltpu.SemaphoreType.DMA((2,))
BLOCK = 2688
HALF = BLOCK // 2
MESH = pl.DeviceIdType.MESH
GATHER = 1, 3, 6, 8, 10, 12, 15, 17


def dot(a, b, over=(1, 0)):
    return lax.dot_general(a, b, (((over[0],), (over[1],)), ((), ())), preferred_element_type=F32)


def at(step, size):
    return pl.ds(pl.multiple_of(step * size, size), size)


def scale_of(h):
    return lax.rsqrt(jnp.mean(h * h, 0, keepdims=True) + EPS)


def turned(source, stage, sems, write):
    chunks = source.shape[0] // EDGE

    def copy(c, slot):
        return pltpu.make_async_copy(source.at[at(c, EDGE), :], stage.at[slot], sems.at[slot])

    copy(0, 0).start()
    copy(1, 1).start()

    def step(c, _):
        for slot in range(2):
            copy(2 * c + slot, slot).wait()
            write(2 * c + slot, stage[slot].T, slot)

            @pl.when(2 * c + slot + 2 < chunks)
            def _():
                copy(2 * c + slot + 2, slot).start()
        return 0

    lax.fori_loop(0, chunks // 2, step, 0)


def forward_kernel(x, gate, up, down, xt_out, at_out, ht_out, at1_out, wg_out, wu_out, wd_out, gu_out, *refs):
    wg, wu, wd, a, total, p, stage, turn, both, sems, osems, own, done, ssem, rsem, tsem, bsem = refs
    n, passes = pl.program_id(0), pl.num_programs(0)
    chunks, tiles = a.shape[1] // CHUNK, wg.shape[0]
    s, r = lax.axis_index("s"), lax.axis_index("r")
    core = s % 2
    partner, across, beside = {"s": s + 1 - 2 * core}, {"s": (s + 2) % 4}, {"r": 1 - r}
    there = (s + 2) % 4

    def rows(ref, size, owner, half=None):
        if half is None:
            return pl.ds(pl.multiple_of(owner * size, size), size)
        return pl.ds(pl.multiple_of(owner * size + half * (size // 2), 16), size // 2)

    def sent(flow, j, device, owner, half=None):
        for ref, size in ((wg, 224), (wu, 224), (wd, 128)):
            part = ref.at[j, rows(ref, size, owner, half), :]
            pltpu.make_async_remote_copy(part, part, ssem.at[flow, j], rsem.at[flow, j], device_id=device, device_id_type=MESH).start()

    def came(sem, j, half=False):
        part = wg.at[j, pl.ds(0, 336 if half else 672), :]
        pltpu.make_async_copy(part, part, sem).wait()

    def load(j, _):
        layer, tile = j // passes, j % passes
        for k in range(4):
            columns = pl.ds(pl.multiple_of(640 * k + 128 * tile, 128), 128)
            for source, ref in ((gate, wg), (up, wu)):
                pltpu.make_async_copy(source.at[layer, :, columns], ref.at[j, rows(ref, 224, s), pl.ds(128 * k, 128)], own.at[j]).start()
        pltpu.make_async_copy(down.at[layer, pl.ds(pl.multiple_of(128 * tile, 128), 128), :], wd.at[j, rows(wd, 128, s), :], own.at[j]).start()
        return 0

    def leave(j, _):
        came(own.at[j], j)
        sent(1, j, across, s, r)
        sent(0, j, partner, s)
        return 0

    def stores(j):
        return [pltpu.make_async_copy(ref.at[j], out.at[j], done.at[i, j]) for i, (ref, out) in enumerate(((wg, wg_out), (wu, wu_out), (wd, wd_out)))]

    def complete(j):
        came(rsem.at[0, j], j)
        came(rsem.at[3, j], j)
        for copy in stores(j):
            copy.start()

    def crossed(j):
        came(rsem.at[1, j], j, True)
        sent(2, j, beside, there, r)

    def joined(j):
        came(rsem.at[2, j], j, True)
        sent(3, j, partner, there)

    def kept_x(c, slot):
        return pltpu.make_async_copy(turn.at[slot], xt_out.at[:, at(c, EDGE)], tsem.at[slot])

    def kept_both(c, i):
        tokens = pl.ds(pl.multiple_of(c * CHUNK + i * SUB, SUB), SUB)
        return pltpu.make_async_copy(both.at[c % 2, i], gu_out.at[:, at(n, TILE), tokens], bsem.at[c % 2, i])

    @pl.when(n == 0)
    def _():
        barrier = pltpu.get_barrier_semaphore()
        for device in (partner, across, beside):
            pl.semaphore_signal(barrier, 1, device_id=device, device_id_type=MESH)
        lax.fori_loop(0, tiles, load, 0)
        pl.semaphore_wait(barrier, 3)
        lax.fori_loop(0, tiles, leave, 0)

        def write(c, ht, slot):
            h = ht.astype(F32)

            @pl.when(c >= 2)
            def _():
                kept_x(c - 2, slot).wait()

            turn[slot] = ht
            kept_x(c, slot).start()
            a[:, at(c, EDGE)] = (h * scale_of(h)).astype(BF16)

        turned(x, stage, sems, write)
        for slot in range(2):
            kept_x(a.shape[1] // EDGE - 2 + slot, slot).wait()
        pltpu.make_async_copy(a, at_out, osems.at[1]).start()
        total[:] = jnp.zeros_like(total)
        crossed(0)
        joined(0)
        crossed(1)
        complete(0)

    def further(j):
        if j > 2:
            complete(j - 2)
        if j - 1 < tiles:
            joined(j - 1)
        if j < tiles:
            crossed(j)

    def step(c, _):
        q = n * chunks + c

        @pl.when(q > 1)
        def _():
            for i in range(CHUNK // SUB):
                kept_both(c, i).wait()

        for i in range(CHUNK // SUB):
            tokens = pl.ds(pl.multiple_of(c * CHUNK + i * SUB, SUB), SUB)
            g, u = dot(wg[n], a[:, tokens], TN), dot(wu[n], a[:, tokens], TN)
            both[c % 2, i, 0], both[c % 2, i, 1] = g, u
            p[:, pl.ds(i * SUB, SUB)] = (g * jax.nn.sigmoid(g) * u).astype(BF16)
        total[:, at(c, CHUNK)] += dot(wd[n], p[:], TN)
        for i in range(CHUNK // SUB):
            kept_both(c, i).start()
        for j, when in enumerate(GATHER, 2):
            pl.when(q == when)(functools.partial(further, j))

        return 0

    lax.fori_loop(0, chunks, step, 0)

    @pl.when(n == passes - 1)
    def _():
        pltpu.make_async_copy(a, at_out, osems.at[1]).wait()
        for c in (chunks - 2, chunks - 1):
            for i in range(CHUNK // SUB):
                kept_both(c, i).wait()

        def ended(j, _):
            for copy in stores(j):
                copy.wait()
            for flow in range(4):
                came(ssem.at[flow, j], j, flow in (1, 2))
            return 0

        parts = a.shape[1] // TILE
        lax.fori_loop(0, parts, ended, 0)

        def move(k, back):
            out = (ht_out if back else xt_out).at[:, at(k, TILE)]
            return pltpu.make_async_copy(*((wg.at[k], out) if back else (out, wg.at[k])), own.at[k])

        for k in range(parts):
            move(k, False).start()

        def last(k, _):
            cols = at(k, TILE)
            move(k, False).wait()
            h = (wg[k].astype(F32) + total[:, cols].astype(BF16).astype(F32)).astype(BF16)
            wg[k] = h
            move(k, True).start()
            h = h.astype(F32)
            a[:, cols] = (h * scale_of(h)).astype(BF16)
            return 0

        lax.fori_loop(0, parts, last, 0)
        two = pltpu.make_async_copy(a, at1_out, osems.at[1])
        two.start()
        further(tiles)
        further(tiles + 1)
        lax.fori_loop(parts, tiles, ended, 0)
        for k in range(parts):
            move(k, True).wait()
        two.wait()


def forward(x, gate, up, down):
    tokens, d = x.shape
    state = jax.ShapeDtypeStruct((d, tokens), BF16)
    wide, tall = (10, d, TILE), (10, TILE, d)
    return pl.pallas_call(
        forward_kernel,
        grid=(5,),
        in_specs=[ANY] * 4,
        out_specs=[ANY] * 8,
        out_shape=[state] * 4 + [jax.ShapeDtypeStruct(shape, BF16) for shape in (wide, wide, tall)] + [jax.ShapeDtypeStruct((2, 2560, tokens), F32)],
        scratch_shapes=[
            pltpu.VMEM(wide, BF16),
            pltpu.VMEM(wide, BF16),
            pltpu.VMEM(tall, BF16),
            pltpu.VMEM((d, tokens), BF16),
            pltpu.VMEM((d, tokens), F32),
            pltpu.VMEM((TILE, CHUNK), BF16),
            pltpu.VMEM((2, EDGE, d), BF16),
            pltpu.VMEM((2, d, EDGE), BF16),
            pltpu.VMEM((2, CHUNK // SUB, 2, TILE, SUB), F32),
            PAIR,
            PAIR,
            pltpu.SemaphoreType.DMA((10,)),
            pltpu.SemaphoreType.DMA((3, 10)),
            pltpu.SemaphoreType.DMA((4, 10)),
            pltpu.SemaphoreType.DMA((4, 10)),
            PAIR,
            pltpu.SemaphoreType.DMA((2, 2)),
        ],
        compiler_params=pltpu.CompilerParams(
            vmem_limit_bytes=67043328, dimension_semantics=("arbitrary",), collective_id=0, has_side_effects=True
        ),
        cost_estimate=pl.CostEstimate(flops=6 * tokens * d * 2560, bytes_accessed=60 * 2**20, transcendentals=0),
        name="forward_layer",
    )(x, gate, up, down)


class Exchange:
    def __init__(self, jobs, place_of, accs, bufs, outs, ssem, rsem, free, osem):
        self.jobs, self.place_of, self.accs, self.bufs, self.outs = jobs, place_of, accs, bufs, outs
        self.free, self.osem = free, osem
        kept, keep_x, keep_y, send_d, recv_d, send_x, recv_x, send_y, recv_y, done, done_t = bufs
        s, r = lax.axis_index("s"), lax.axis_index("r")
        self.x, self.core = s // 2, s % 2
        self.devices = {"s": s + 1 - 2 * self.core}, {"s": (s + 2) % 4}, {"r": 1 - r}
        self.mine, self.other = pl.ds(pl.multiple_of(r * HALF, HALF), HALF), pl.ds(pl.multiple_of((1 - r) * HALF, HALF), HALF)
        half = done.at[self.mine, :]
        pairs = (send_d, recv_d, 0), (send_x, recv_x, 1), (send_y, recv_y, 2), (half, half, 2)
        self.to = [self.devices[way] for *_, way in pairs]
        self.copies = [
            pltpu.make_async_remote_copy(source, target, ssem.at[i], rsem.at[i], device_id=self.devices[way], device_id_type=MESH)
            for i, (source, target, way) in enumerate(pairs)
        ]

    def meet(self):
        barrier = pltpu.get_barrier_semaphore()
        for device in self.devices:
            pl.semaphore_signal(barrier, 1, device_id=device, device_id_type=MESH)
        return lambda: pl.semaphore_wait(barrier, 3)

    def send(self, number, job):
        @pl.when(job > 0)
        def _():
            pl.semaphore_wait(self.free.at[number], 1)

        self.copies[number].start()

    def arrived(self, number):
        self.copies[number].wait_recv()
        self.copies[number].wait_send()

    def freed(self, number, job):
        @pl.when(job < self.jobs - 1)
        def _():
            pl.semaphore_signal(self.free.at[number], 1, device_id=self.to[number], device_id_type=MESH)

    def pack(self):
        accg, accu, accd = self.accs
        kept, send_d = self.bufs[0], self.bufs[3]

        def cut(owner, ref, slot):
            rows = pl.ds(pl.multiple_of(owner * 224, 32), 224)
            for k in range(4):
                ref[slot, k * 224 : k * 224 + 224, :] = accg[rows, k * 128 : k * 128 + 128].astype(ref.dtype)
                ref[slot, 896 + k * 224 : 1120 + k * 224, :] = accu[rows, k * 128 : k * 128 + 128].astype(ref.dtype)
            ref[slot, 1792:, :] = accd[:, pl.ds(pl.multiple_of(owner * 128, 128), 128)].astype(ref.dtype)

        for slot, place in ((0, self.x), (1, 1 - self.x)):
            cut(2 * place + self.core, kept, slot)
            cut(2 * place + 1 - self.core, send_d, slot)

    def after_partner(self, job):
        kept, keep_x, _, _, recv_d, send_x, *_ = self.bufs
        self.arrived(0)
        send_x[:] = (kept[1] + recv_d[1].astype(F32)).astype(BF16)
        keep_x[:] = kept[0] + recv_d[0].astype(F32)
        self.freed(0, job)
        self.send(1, job)

    def after_across(self, job):
        _, keep_x, keep_y, _, _, _, recv_x, send_y, *_ = self.bufs
        self.arrived(1)
        keep_y[:] = keep_x[self.mine, :] + recv_x[self.mine, :].astype(F32)
        send_y[:] = (keep_x[self.other, :] + recv_x[self.other, :].astype(F32)).astype(BF16)
        self.freed(1, job)
        self.send(2, job)

    def after_beside(self, job):
        keep_y, recv_y, done = self.bufs[2], self.bufs[8], self.bufs[9]
        self.arrived(2)
        done[self.mine, :] = (keep_y[:] + recv_y[:].astype(F32)).astype(BF16)
        self.freed(2, job)
        self.send(3, job)

    def whole(self, job):
        done, done_t = self.bufs[9:]
        self.arrived(3)
        layer, tile = self.place_of(job)
        done_t[:] = done[1792:, :].T
        for i, out in enumerate(self.outs[:2]):
            for k in range(4):
                columns = pl.ds(pl.multiple_of(640 * k + 128 * tile, 128), 128)
                pltpu.make_async_copy(done.at[pl.ds(896 * i + 224 * k, 224), :], out.at[layer, :, columns], self.osem).start()
        pltpu.make_async_copy(done_t, self.outs[2].at[layer, pl.ds(pl.multiple_of(128 * tile, 128), 128), :], self.osem).start()

    def written(self, job):
        done = self.bufs[9]
        pltpu.make_async_copy(done, done, self.osem).wait()
        self.freed(3, job)


EXCHANGE = [
    pltpu.VMEM((2, BLOCK, 128), F32),
    pltpu.VMEM((BLOCK, 128), F32),
    pltpu.VMEM((HALF, 128), F32),
    pltpu.VMEM((2, BLOCK, 128), BF16),
    pltpu.VMEM((2, BLOCK, 128), BF16),
    pltpu.VMEM((BLOCK, 128), BF16),
    pltpu.VMEM((BLOCK, 128), BF16),
    pltpu.VMEM((HALF, 128), BF16),
    pltpu.VMEM((HALF, 128), BF16),
    pltpu.VMEM((BLOCK, 128), BF16),
    pltpu.VMEM((128, 896), BF16),
    pltpu.SemaphoreType.DMA((4,)),
    pltpu.SemaphoreType.DMA((4,)),
    pltpu.SemaphoreType.REGULAR((4,)),
    pltpu.SemaphoreType.DMA,
]


def elementwise(g, u, dp):
    dp = dp.astype(BF16).astype(F32)
    sg = jax.nn.sigmoid(g)
    t = g * sg
    return (t * u).astype(BF16), (dp * u * (sg + t * (1 - sg))).astype(BF16), (dp * t).astype(BF16)


def through_norm(da, h, by):
    da, h = da.astype(BF16).astype(F32), h.astype(F32)
    f = scale_of(h)
    dh = (f * da - h * (f * f * f * jnp.mean(da * h, 0, keepdims=True))).astype(BF16)
    return (by.astype(F32) + dh.astype(F32)).astype(BF16)


def last_kernel(at_in, ht_in, by_in, wg, wu, wd, by_out, og, ou, od, kept_out, sent_out, *refs):
    a, by, total, *accs, p, dg, du, stage, sems, osems = refs[:12]
    ex = Exchange(4, lambda job: (1, job), accs, refs[12:23], (og, ou, od), *refs[23:])
    kept, send_d = ex.bufs[0], ex.bufs[3]
    accg, accu, accd = accs
    n, passes = pl.program_id(0), pl.num_programs(0)
    chunks, steps = a.shape[1] // CHUNK, a.shape[1] // EDGE
    job = n - 1

    @pl.when(n == 0)
    def _():
        met = ex.meet()
        one = pltpu.make_async_copy(at_in, a, osems.at[0])
        one.start()
        met()

        def write(c, t, slot):
            by[:, at(c, EDGE)] = t

        turned(by_in, stage, sems, write)
        total[:] = jnp.zeros_like(total)
        one.wait()

    for acc in accs:
        acc[:] = jnp.zeros_like(acc)

    def step(c, _):
        cols = at(c, CHUNK)
        gate, up, down = wg[:], wu[:], wd[:]
        for i in range(CHUNK // SUB):
            tokens, q = pl.ds(pl.multiple_of(c * CHUNK + i * SUB, SUB), SUB), pl.ds(i * SUB, SUB)
            g, u = dot(gate, a[:, tokens], TN), dot(up, a[:, tokens], TN)
            p[:, q], dg[:, q], du[:, q] = elementwise(g, u, dot(down, by[:, tokens]))
        total[:, cols] += dot(gate, dg[:]) + dot(up, du[:])
        accg[:] += dot(a[:, cols], dg[:], NT)
        accu[:] += dot(a[:, cols], du[:], NT)
        accd[:] += dot(by[:, cols], p[:], NT)

        @pl.when((c == 0) & (job >= 0))
        def _():
            ex.after_partner(job)

        @pl.when((c == 0) & (job >= 1))
        def _():
            ex.whole(job - 1)

        @pl.when((c == 1) & (job >= 1))
        def _():
            ex.written(job - 1)

        @pl.when((c == 2) & (job >= 0))
        def _():
            ex.after_across(job)

        return 0

    lax.fori_loop(0, chunks, step, 0)

    @pl.when(job >= 0)
    def _():
        ex.after_beside(job)

    ex.pack()

    @pl.when(n < passes - 1)
    def _():
        ex.send(0, job + 1)

    @pl.when(n == passes - 1)
    def _():
        one = pltpu.make_async_copy(ht_in, a, osems.at[0])
        one.start()
        three, four = pltpu.make_async_copy(kept, kept_out, sems.at[0]), pltpu.make_async_copy(send_d, sent_out, sems.at[1])
        three.start(), four.start()
        one.wait()

        def last(c, _):
            cols = at(c, EDGE)
            by[:, cols] = through_norm(total[:, cols], a[:, cols], by[:, cols])
            return 0

        lax.fori_loop(0, steps, last, 0)
        two = pltpu.make_async_copy(by, by_out, osems.at[1])
        two.start()
        ex.whole(3)
        ex.written(3)
        three.wait(), four.wait()
        two.wait()


def first_kernel(at_in, ht_in, by_in, gu_in, wg_in, wu_in, wd, kept_in, sent_in, _g, _u, _d, by_out, og, ou, od, dgu_out, *refs):
    a, by, *accs, gu, p, dgu, wgs, wus, dgb, stage, sems, osems, gsem, dsem, lsem, wsem = refs[:18]
    ex = Exchange(6, lambda job: (1 - (job + 4) // 5, (job + 4) % 5), accs, refs[18:29], (og, ou, od), *refs[29:])
    kept, send_d = ex.bufs[0], ex.bufs[3]
    accg, accu, accd = accs
    n, passes = pl.program_id(0), pl.num_programs(0) - 1
    chunks, steps = a.shape[1] // CHUNK, a.shape[1] // EDGE

    def brought(q, slot):
        return pltpu.make_async_copy(gu_in.at[:, at(q // chunks, TILE), at(q % chunks, CHUNK)], gu.at[slot], gsem.at[slot])

    def stored(q, slot):
        return pltpu.make_async_copy(dgu.at[slot], dgu_out.at[:, at(q // chunks, TILE), at(q % chunks, CHUNK)], dsem.at[slot])

    def matrix(tile, i):
        return pltpu.make_async_copy((wg_in, wu_in)[i].at[tile], (wgs, wus)[i].at[:, pl.ds(tile * TILE, TILE)], wsem.at[i, tile])

    @pl.when(n == 0)
    def _():
        met = ex.meet()
        three, four = pltpu.make_async_copy(kept_in, kept, sems.at[0]), pltpu.make_async_copy(sent_in, send_d, sems.at[1])
        three.start(), four.start()
        brought(0, 0).start()
        one, two = pltpu.make_async_copy(at_in, a, osems.at[0]), pltpu.make_async_copy(by_in, by, osems.at[1])
        two.start(), one.start()
        for tile in range(5):
            matrix(tile, 0).start(), matrix(tile, 1).start()
        three.wait(), four.wait()
        met()
        ex.send(0, n)
        two.wait(), one.wait()

    @pl.when(n < passes)
    def _():
        for acc in accs:
            acc[:] = jnp.zeros_like(acc)

        def step(c, _):
            q, slot = n * chunks + c, c % 2
            cols = at(c, CHUNK)
            brought(q, slot).wait()

            @pl.when(q + 1 < passes * chunks)
            def _():
                brought(q + 1, 1 - slot).start()

            @pl.when(q >= 2)
            def _():
                stored(q - 2, slot).wait()

            for i in range(CHUNK // SUB):
                tokens, b = pl.ds(pl.multiple_of(c * CHUNK + i * SUB, SUB), SUB), pl.ds(i * SUB, SUB)
                p[:, b], dgu[slot, 0, :, b], dgu[slot, 1, :, b] = elementwise(gu[slot, 0, :, b], gu[slot, 1, :, b], dot(wd[:], by[:, tokens]))
            accg[:] += dot(a[:, cols], dgu[slot, 0], NT)
            accu[:] += dot(a[:, cols], dgu[slot, 1], NT)
            accd[:] += dot(by[:, cols], p[:], NT)
            stored(q, slot).start()

            @pl.when((c == 0) & (n >= 2))
            def _():
                ex.whole(n - 2)

            @pl.when((c == 0) & (n >= 1))
            def _():
                ex.after_across(n - 1)

            @pl.when(c == 0)
            def _():
                ex.after_partner(n)

            @pl.when((c == 1) & (n >= 2))
            def _():
                ex.written(n - 2)

            @pl.when((c == 2) & (n >= 1))
            def _():
                ex.after_beside(n - 1)

            return 0

        lax.fori_loop(0, chunks, step, 0)
        ex.pack()
        ex.send(0, n + 1)

    @pl.when(n == passes)
    def _():
        one = pltpu.make_async_copy(ht_in, a, osems.at[0])
        one.start()
        for slot in range(2):
            stored(passes * chunks - 2 + slot, slot).wait()

        def brought_back(c, slot):
            return pltpu.make_async_copy(dgu_out.at[:, :, at(c, EDGE)], dgb.at[slot], lsem.at[slot])

        def copy(c, slot):
            return pltpu.make_async_copy(stage.at[slot], by_out.at[at(c, EDGE), :], sems.at[slot])

        brought_back(0, 0).start()
        for tile in range(5):
            matrix(tile, 0).wait(), matrix(tile, 1).wait()
        one.wait()

        def opening():
            ex.whole(3)
            ex.after_across(4)
            ex.after_partner(5)

        hooks = {
            0: opening,
            1: lambda: ex.written(3),
            4: lambda: ex.after_beside(4),
            7: lambda: ex.after_across(5),
            8: lambda: ex.whole(4),
            9: lambda: ex.written(4),
            11: lambda: ex.after_beside(5),
        }

        def step(c, _):
            slot, cols = c % 2, at(c, EDGE)
            brought_back(c, slot).wait()

            @pl.when(c + 1 < steps)
            def _():
                brought_back(c + 1, 1 - slot).start()

            da = dot(wgs[:], dgb[slot, 0]) + dot(wus[:], dgb[slot, 1])

            @pl.when(c >= 2)
            def _():
                copy(c - 2, slot).wait()

            stage[slot] = through_norm(da, a[:, cols], by[:, cols]).T
            copy(c, slot).start()
            for at_step, hook in hooks.items():
                pl.when(c == at_step)(hook)
            return 0

        lax.fori_loop(0, steps, step, 0)
        copy(steps - 2, 0).wait()
        copy(steps - 1, 1).wait()
        ex.whole(5)
        ex.written(5)


def params(number):
    return pltpu.CompilerParams(vmem_limit_bytes=67043328, dimension_semantics=("arbitrary",), collective_id=number, has_side_effects=True)


def gradients():
    return [jax.ShapeDtypeStruct(shape, BF16) for shape in ((2, 224, 2560), (2, 224, 2560), (2, 640, 896))]


def backward_last(a, h, by, weights):
    d, tokens = a.shape
    return pl.pallas_call(
        last_kernel,
        grid=(5,),
        in_specs=[ANY, ANY, ANY] + [pl.BlockSpec((None, *w.shape[1:]), lambda n: (5 + n, 0, 0)) for w in weights],
        out_specs=[ANY] * 6,
        out_shape=[jax.ShapeDtypeStruct((d, tokens), BF16), *gradients(), jax.ShapeDtypeStruct((2, BLOCK, 128), F32), jax.ShapeDtypeStruct((2, BLOCK, 128), BF16)],
        scratch_shapes=[
            pltpu.VMEM((d, tokens), BF16),
            pltpu.VMEM((d, tokens), BF16),
            pltpu.VMEM((d, tokens), F32),
            *[pltpu.VMEM((d, TILE), F32)] * 3,
            *[pltpu.VMEM((TILE, CHUNK), BF16)] * 3,
            pltpu.VMEM((2, EDGE, d), BF16),
            PAIR,
            PAIR,
            *EXCHANGE,
        ],
        compiler_params=params(1),
        cost_estimate=pl.CostEstimate(flops=16 * tokens * d * 2560, bytes_accessed=60 * 2**20, transcendentals=0),
        name="backward_last",
    )(a, h, by, *weights)


def backward_first(a, h, by, gu, weights, kept, sent, sums):
    d, tokens = a.shape
    return pl.pallas_call(
        first_kernel,
        grid=(6,),
        in_specs=[ANY] * 6 + [pl.BlockSpec((None, TILE, d), lambda n: (n - n // 5, 0, 0))] + [ANY] * 5,
        out_specs=[ANY] * 5,
        out_shape=[jax.ShapeDtypeStruct((tokens, d), BF16), *gradients(), jax.ShapeDtypeStruct((2, 2560, tokens), BF16)],
        input_output_aliases={9: 1, 10: 2, 11: 3},
        scratch_shapes=[
            pltpu.VMEM((d, tokens), BF16),
            pltpu.VMEM((d, tokens), BF16),
            *[pltpu.VMEM((d, TILE), F32)] * 3,
            pltpu.VMEM((2, 2, TILE, CHUNK), F32),
            pltpu.VMEM((TILE, CHUNK), BF16),
            pltpu.VMEM((2, 2, TILE, CHUNK), BF16),
            pltpu.VMEM((d, 2560), BF16),
            pltpu.VMEM((d, 2560), BF16),
            pltpu.VMEM((2, 2, 2560, EDGE), BF16),
            pltpu.VMEM((2, EDGE, d), BF16),
            PAIR,
            PAIR,
            PAIR,
            PAIR,
            PAIR,
            pltpu.SemaphoreType.DMA((2, 5)),
            *EXCHANGE,
        ],
        compiler_params=params(2),
        cost_estimate=pl.CostEstimate(flops=12 * tokens * d * 2560, bytes_accessed=200 * 2**20, transcendentals=0),
        name="backward_first",
    )(a, h, by, gu, *weights, kept, sent, *sums)


def solution(mesh):
    def step(x, dy, *weights):
        xt, a0, h1, a1, *whole, gu = forward(x[0], *weights)
        by_h1, *sums, kept, sent = backward_last(a1, h1, dy[0], whole)
        by_x, *sums, _ = backward_first(a0, xt, by_h1, gu, whole, kept, sent, sums)
        return by_x[None], *sums

    states, cut = P(("rep", "r", "s"), None, None), P(None, "s", None)
    return jax.shard_map(
        step,
        mesh=mesh,
        in_specs=(states, states) + (cut,) * 3,
        out_specs=(states,) + (P("rep", "s", None),) * 3,
        check_vma=False,
    )
```
